32 devices in a mesh: section: 4 (over y, core), fsdp: 8 (over z, x).
Axes of the slice: x: 2, y: 2, z: 4, core: 2. Of those that a mesh axis runs over, the one named last changes fastest.
Arguments:
- old_pieces: bfloat16 [4, 2, 16384, 1024], P('section', None, 'fsdp'), may hold values from -0.0625 to 0.0625
- section_inputs: bfloat16 [4, 4096, 8192], P('section', 'fsdp'), may hold values from -6 to 6
- old_section_of: int32 [8], replicated, may hold values from 0 to 3, as said below
- new_section_of: int32 [8], replicated, may hold values from 0 to 7, as said below
- old_order: int32 [8, 2], replicated, may hold values from 0 to 1, each once within a row
- new_order: int32 [8, 2], replicated, may hold values from 0 to 1, each once within a row
Outputs:
- new_shards: bfloat16 [4, 32768, 1024], P('section', 'fsdp')
- kv_out: bfloat16 [4, 4096, 2048], P('section', 'fsdp')
The draws below stay inside these ranges and needn't reach their ends.
Inputs may be any that keep to these rules, and one draw needn't show every extreme that they name: `old_section_of`: each old section holds exactly two layers. Each new section holds exactly one layer; the two layers of one old section have different values of new_section_of // 2.
All inputs are finite; a program needn't handle non-finite values.
Results may differ from the reference program's by a relative error of at most 0.001.
Values may be sent and summed in bfloat16 or wider, within the bound.
A program may use at most 192 MiB of HBM per device.

```python
import math
import jax
import jax.numpy as jnp
from jax import lax

D = 8192
HEAD_DIM = 128
TOK_DEV = 512
KVW = 1024
LAYERS = 8
SHARD = 4096
N_SECTION = 4
N_FSDP = 8


def layer_maps(key):
    section_count = N_SECTION
    keys = jax.random.split(jax.random.fold_in(key, 11), 6)
    members = jax.random.permutation(keys[0], 2 * section_count).astype(jnp.int32)
    old_section = (jnp.argsort(members) // 2).astype(jnp.int32)
    rows_first = jax.random.permutation(keys[1], section_count).astype(jnp.int32)
    relabel = jax.random.permutation(keys[2], section_count).astype(jnp.int32)
    offset_steps = jax.random.randint(keys[3], (), 1, section_count).astype(jnp.int32)
    relabel_inverse = jnp.argsort(relabel).astype(jnp.int32)
    rows_second = rows_first[relabel_inverse[(relabel + offset_steps) % section_count]]
    swapped = jax.random.randint(keys[4], (section_count,), 0, 2).astype(jnp.int32)
    layer_alpha = jnp.where(swapped == 0, members[0::2], members[1::2])
    layer_beta = jnp.where(swapped == 0, members[1::2], members[0::2])
    halves = jax.random.randint(keys[5], (section_count,), 0, 2).astype(jnp.int32)
    section_alpha = 2 * rows_first + halves[rows_first]
    section_beta = 2 * rows_second + 1 - halves[rows_second]
    new_section = jnp.zeros((2 * section_count,), jnp.int32).at[layer_alpha].set(section_alpha).at[layer_beta].set(section_beta)
    return (old_section, new_section)


def draw_old_section_of(key, part):
    return layer_maps(key)[0]


def draw_new_section_of(key, part):
    return layer_maps(key)[1]


def levels(stream_key, dims, shards, low, high):
    factor_of = 1.0
    for dim, parts in shards:
        heights = jax.random.uniform(jax.random.fold_in(jax.random.fold_in(stream_key, 6), dim), (parts,), jnp.float32, low / len(shards), high / len(shards))
        factor_of = factor_of * jnp.repeat(jnp.exp(heights), dims[dim] // parts).reshape((-1,) + (1,) * (len(dims) - 1 - dim))
    return factor_of


def noise(key, extent, deviation, most, shards=(), kind=jnp.bfloat16):
    level = levels(key, extent, shards, -0.22, 0.18) if shards else 1.0
    result = jax.random.normal(key, extent, jnp.float32) * deviation * level
    return jnp.minimum(jnp.maximum(result, -most), most).astype(kind)


def setup_inputs(seed: int = 0) -> dict:
    streams_of = jax.random.split(jax.random.key(seed), 7)
    return {
        "old_pieces": noise(streams_of[0], (N_SECTION, 2, 2 * D, KVW), D ** -0.5, 0.0625, ((0, 4), (2, 8))),
        "section_inputs": noise(streams_of[1], (N_SECTION, N_FSDP * TOK_DEV, D), 1.0, 6.0, ((0, 4), (1, 8))),
        "old_section_of": draw_old_section_of(jax.random.fold_in(streams_of[6], 71), 0),
        "new_section_of": draw_new_section_of(jax.random.fold_in(streams_of[6], 71), 0),
        "old_order": jax.vmap(lambda own: jax.random.permutation(own, 2))(jax.random.split(streams_of[4], LAYERS)).reshape((LAYERS, 2)).astype(jnp.int32),
        "new_order": jax.vmap(lambda own: jax.random.permutation(own, 2))(jax.random.split(streams_of[5], LAYERS)).reshape((LAYERS, 2)).astype(jnp.int32),
    }


def rotate_keys(values, positions):
    tok_rows = values.shape[0]
    heads = values.reshape(tok_rows, -1, HEAD_DIM)
    half_dim = HEAD_DIM // 2
    freq_index = jnp.arange(half_dim, dtype=jnp.float32)
    inverse_freq = jnp.exp(freq_index * (-2.0 * math.log(500000.0) / HEAD_DIM))
    angles = positions.astype(jnp.float32)[:, None] * inverse_freq[None, :]
    cosine = jnp.cos(angles)[:, None, :]
    sine = jnp.sin(angles)[:, None, :]
    lower = heads[..., :half_dim]
    upper = heads[..., half_dim:]
    turned = jnp.concatenate([lower * cosine - upper * sine, upper * cosine + lower * sine], axis=-1)
    return turned.reshape(tok_rows, -1)


def reference(old_pieces, section_inputs, old_section_of, new_section_of, old_order, new_order):
    layer_ids = jnp.arange(LAYERS, dtype=jnp.int32)
    group_size = N_FSDP // 2
    shard_list = []
    output_list = []
    for row_index in range(N_SECTION):
        shard_halves = []
        output_halves = []
        for half in range(2):
            layer_index = jnp.sum(jnp.where(new_section_of == 2 * row_index + half, layer_ids, 0)).astype(jnp.int32)
            old_section = old_section_of[layer_index]
            slot_index = jnp.sum(((old_section_of == old_section) & (layer_ids < layer_index)).astype(jnp.int32))
            flat_rows = old_pieces[old_section, slot_index]
            key_weight = lax.dynamic_slice_in_dim(flat_rows, (old_order[layer_index, 0] * D).astype(jnp.int32), D, 0)
            value_weight = lax.dynamic_slice_in_dim(flat_rows, (old_order[layer_index, 1] * D).astype(jnp.int32), D, 0)
            new_flat = jnp.where(new_order[layer_index, 0] == 0,
                                 jnp.concatenate([key_weight, value_weight], axis=0),
                                 jnp.concatenate([value_weight, key_weight], axis=0))
            shard_halves.append(new_flat.reshape(group_size, SHARD, KVW))
            tokens = section_inputs[row_index].reshape(group_size, 2, TOK_DEV, D)[:, half].reshape(group_size * TOK_DEV, D)
            keys = jnp.dot(tokens, key_weight, preferred_element_type=jnp.float32)
            values = jnp.dot(tokens, value_weight, preferred_element_type=jnp.float32)
            positions = jnp.arange(group_size * TOK_DEV, dtype=jnp.int32)
            joined = jnp.concatenate([rotate_keys(keys, positions), values], axis=-1).astype(jnp.bfloat16)
            output_halves.append(joined.reshape(group_size, TOK_DEV, 2 * KVW))
        shard_list.append(jnp.stack(shard_halves, axis=1).reshape(4 * D, KVW))
        output_list.append(jnp.stack(output_halves, axis=1).reshape(N_FSDP * TOK_DEV, 2 * KVW))
    return jnp.stack(shard_list), jnp.stack(output_list)
```

```python
import math

import jax
import jax.numpy as jnp
from jax import lax
from jax.sharding import PartitionSpec as P


HEAD_DIM = 128


def from_partner(block, axis, stride):
    count = lax.axis_size(axis)
    route = []
    for low in range(count):
        high = low | 1 << stride
        if high != low and high < count:
            route += [(low, high), (high, low)]
    return lax.ppermute(block, axis, route)


def from_offset(block, axis, offset):
    count = lax.axis_size(axis)
    return lax.ppermute(block, axis, [(i, i ^ offset) for i in range(count)])


def rotate_keys(values, positions):
    tok_rows = values.shape[0]
    heads = values.reshape(tok_rows, -1, HEAD_DIM)
    half_dim = HEAD_DIM // 2
    freq_index = jnp.arange(half_dim, dtype=jnp.float32)
    inverse_freq = jnp.exp(freq_index * (-2.0 * math.log(500000.0) / HEAD_DIM))
    angles = positions.astype(jnp.float32)[:, None] * inverse_freq[None, :]
    cosine = jnp.cos(angles)[:, None, :]
    sine = jnp.sin(angles)[:, None, :]
    lower = heads[..., :half_dim]
    upper = heads[..., half_dim:]
    turned = jnp.concatenate(
        [lower * cosine - upper * sine, upper * cosine + lower * sine], axis=-1
    )
    return turned.reshape(tok_rows, -1)


def pick_entry(table, index_value):
    positions = jnp.arange(table.shape[0], dtype=jnp.int32)
    return jnp.sum(jnp.where(positions == index_value, table, 0))


def pick_row(table, index_value):
    positions = jnp.arange(table.shape[0], dtype=jnp.int32)[:, None]
    return jnp.sum(jnp.where(positions == index_value, table, 0), axis=0)


def chunk_columns(kv_width):
    heads = kv_width // HEAD_DIM
    edge = [1, 1] if heads >= 4 else []
    middle = heads - len(edge)
    sizes = [2] * (middle // 2) + [1] * (middle % 2) + edge
    starts = [sum(sizes[:i]) for i in range(len(sizes))]
    return [(s * HEAD_DIM, n * HEAD_DIM) for s, n in zip(starts, sizes)]


def per_device(old_pieces, section_inputs, old_section_of, new_section_of, old_order, new_order):
    section_count = lax.axis_size("section")
    member_count = lax.axis_size("fsdp")
    digit_count = member_count.bit_length() - 1
    row_index = lax.axis_index("section")
    member = lax.axis_index("fsdp")
    parity = member % 2
    layer_total = old_section_of.shape[0]
    layer_ids = jnp.arange(layer_total, dtype=jnp.int32)
    in_row = old_section_of == row_index
    layer_low = jnp.min(jnp.where(in_row, layer_ids, layer_total))
    layer_high = jnp.max(jnp.where(in_row, layer_ids, -1))
    target_low = pick_entry(new_section_of, layer_low) // 2
    layer_own = jnp.sum(jnp.where(new_section_of == 2 * row_index + parity, layer_ids, 0))
    layer_foreign = jnp.sum(jnp.where(new_section_of == 2 * row_index + 1 - parity, layer_ids, 0))
    source_own = pick_entry(old_section_of, layer_own)
    source_foreign = pick_entry(old_section_of, layer_foreign)
    pieces = old_pieces[0]
    tokens = section_inputs[0]
    tok_rows, _ = tokens.shape
    shard_rows, kv_width = 2 * pieces.shape[1], pieces.shape[2]
    own_bits = {digit: member // 2**digit % 2 for digit in range(1, digit_count)}
    own_old = pick_row(old_order, layer_own)
    own_new = pick_row(new_order, layer_own)
    flipped = own_old[0] != own_new[0]
    group_digits = digit_count - 1
    low_count = group_digits // 2
    high_digits = list(range(low_count + 1, digit_count))
    low_digits = list(range(1, low_count + 1))
    top_bit = own_bits[digit_count - 1]

    def to_groups(low, high):
        sources = []
        for offset in range(section_count):
            chosen = jnp.where(target_low == row_index ^ offset, low, high)
            if offset:
                chosen = from_offset(chosen, "section", offset)
            sources.append(chosen)
        (own_from, foreign_from, here, side), sources = lax.optimization_barrier(
            ((source_own, source_foreign, row_index, parity), sources)
        )
        own, foreign = sources[0], sources[0]
        for offset in range(1, section_count):
            own = jnp.where(own_from == here ^ offset, sources[offset], own)
            foreign = jnp.where(foreign_from == here ^ offset, sources[offset], foreign)
        partner = from_partner(foreign, "fsdp", 0)
        lower = jnp.where(side == 0, own, partner)
        upper = jnp.where(side == 0, partner, own)
        return jnp.concatenate([lower, upper], axis=-2)

    def gather_high(block):
        blocks = [block]
        for digit in high_digits:
            blocks += [from_partner(held, "fsdp", digit) for held in blocks]
        return blocks

    block_digits = high_digits[:-1]
    place_digits = block_digits[::-1] + low_digits[::-1]

    def pick_columns(flips):
        column = 0
        for digit in place_digits:
            column = 2 * column + (own_bits[digit] ^ flips[digit])
        return lax.dynamic_slice_in_dim(tokens, column * shard_rows, shard_rows, axis=1)

    row_cuts = 4 if tok_rows % 64 == 0 else 1
    token_blocks = {}
    for number in range(2 ** len(block_digits)):
        flips = {digit: number >> place & 1 for place, digit in enumerate(block_digits)}
        pending = {}
        for want in range(2**low_count):
            low_flips = {digit: want >> place & 1 for place, digit in enumerate(low_digits)}
            pending[want] = pick_columns({**flips, **low_flips})
        for place, digit in enumerate(low_digits):
            moved = dict(pending)
            for want in range(2**low_count):
                if want >> place & 1:
                    cuts = jnp.split(pending[want], row_cuts, axis=0)
                    cuts = [from_partner(cut, "fsdp", digit) for cut in cuts]
                    moved[want] = jnp.concatenate(cuts, axis=0)
            pending = moved
        for want in range(2**low_count):
            token_blocks[want, number] = pending[want]

    def project(blocks):
        sums = []
        for want in reversed(range(2**low_count)):
            for number, block in enumerate(blocks):
                product = jnp.dot(
                    token_blocks[want, number], block, preferred_element_type=jnp.float32
                )
                total = total + product if number else product
            sums.append(total)
        sums = sums[::-1]
        for place in reversed(range(low_count)):
            half = len(sums) // 2
            sums = [
                kept + from_partner(sent, "fsdp", low_digits[place])
                for kept, sent in zip(sums[:half], sums[half:])
            ]
        return sums[0]

    positions = member // 2 * tok_rows + jnp.arange(tok_rows, dtype=jnp.int32)
    shard_parts, key_parts, value_parts = [], [], []
    for number, (start, width) in enumerate(chunk_columns(kv_width)):
        part = lax.slice_in_dim(pieces, start, start + width, axis=2)
        if number == 0:
            crossed = jnp.stack(gather_high(part), axis=1)
            held = to_groups(crossed[0], crossed[1])
            blocks = [held[i] for i in range(held.shape[0])]
        else:
            blocks = gather_high(to_groups(part[0], part[1]))
        half = len(blocks) // 2
        near = project(blocks[:half])
        far = project(blocks[half:])
        shard_parts.append(jnp.where(flipped, blocks[half], blocks[0]))
        keys = jnp.where(own_old[0] == top_bit, near, far)
        values = jnp.where(own_old[1] == top_bit, near, far)
        key_parts.append(rotate_keys(keys, positions).astype(jnp.bfloat16))
        value_parts.append(values.astype(jnp.bfloat16))
    new_shard = jnp.concatenate(shard_parts, axis=1)
    joined = jnp.concatenate(key_parts + value_parts, axis=1)
    return (new_shard[None], joined[None])


def solution(mesh):
    in_specs = (P("section", None, "fsdp", None), P("section", "fsdp", None), P(), P(), P(), P())
    out_specs = (P("section", "fsdp", None), P("section", "fsdp", None))

    return jax.shard_map(
        per_device, mesh=mesh, in_specs=in_specs, out_specs=out_specs, check_vma=False
    )
```
